256 devices in a mesh: group: 4 (over y, x), row: 64 (over z, core).
Axes of the slice: x: 2, y: 2, z: 32, core: 2. Of those that a mesh axis runs over, the one named last changes fastest.
The devices are a block of a 4x8x32 slice.
Arguments:
- pair_repr: bfloat16 [2048, 512, 128], P(('group', 'row')), parts along dimension 0, may hold values from -60 to 60
- proj_weight: bfloat16 [128, 512], replicated, may hold values from -1.25 to 1.25
- gate_bias: float32 [128], replicated, may hold values from -4 to 4
- bias_weight: bfloat16 [128, 4], replicated, may hold values from -8 to 8
- out_weight: bfloat16 [128, 128], replicated, may hold values from -0.5 to 0.5
- out_bias: float32 [128], replicated, may hold values from -1.5 to 1.5
Outputs:
- pair_update: bfloat16 [2048, 512, 128], P(('group', 'row')), parts along dimension 0
The draws below stay inside these ranges and needn't reach their ends.
There are 4 independent parts, one for each index of `group`. The reference program is written for one: setup_inputs(seed, part) draws one part's arguments, and reference() takes and returns one part's arrays. A program takes and returns all parts, laid end to end along the dimension named above; an argument that names none is the same for every part. Nothing has to cross between parts.
All inputs are finite; a program needn't handle non-finite values.
Results may differ from the reference program's by a relative error of at most 0.0085.
The reference program's roundings to bfloat16 on the way (of `normed`, `weights` and `gated`) count: a program that leaves them out, or rounds other values in their place, can miss the bound.
Values may be sent and summed in bfloat16 or wider, within the bound.
A program may use at most 64 MiB of HBM per device.

```python
import math
import jax
import jax.numpy as jnp
from jax import lax

C = 128
HEADS = 4
INNER = 128
N = 512


def draw_pair_repr(key, part):
    entries = jax.random.normal(jax.random.fold_in(key, 1), (N, N, C), jnp.float32)
    entries = jnp.clip(entries, -6.0, 6.0)
    return entries.astype(jnp.bfloat16)


def draw_bias_weight(key, part):
    result = jnp.clip(jax.random.normal(jax.random.fold_in(key, 13), (C, HEADS), jnp.float32), -4.0, 4.0) * (2.0 / math.sqrt(C))
    return result.astype(jnp.bfloat16)


def bell_draw(rng, shape, scale, bound, kind=jnp.bfloat16):
    drawn = jax.random.normal(rng, shape, jnp.float32) * scale
    return jnp.minimum(jnp.maximum(drawn, -bound), bound).astype(kind)


def setup_inputs(seed: int = 0, part: int = 0) -> dict:
    streams_of = jax.random.split(jax.random.key(seed), 7)
    part_keys = jax.random.split(jax.random.fold_in(streams_of[6], part), 7)
    pair_repr = draw_pair_repr(jax.random.fold_in(jax.random.fold_in(streams_of[6], part), 71), part)
    proj_weight = bell_draw(streams_of[1], (C, 4 * INNER), (C // 5) ** -0.5, 1.25)
    gate_bias = bell_draw(streams_of[2], (INNER,), 1.0, 4.0, jnp.float32)
    bias_weight = draw_bias_weight(jax.random.fold_in(streams_of[6], 71), part)
    out_weight = bell_draw(streams_of[4], (INNER, C), INNER ** -0.5, 0.5)
    out_bias = bell_draw(streams_of[5], (C,), 0.3, 1.5, jnp.float32)
    return {"pair_repr": pair_repr, "proj_weight": proj_weight, "gate_bias": gate_bias, "bias_weight": bias_weight, "out_weight": out_weight, "out_bias": out_bias}


EPSILON = 1e-05

def normalize(pair_repr):
    values_f = pair_repr.astype(jnp.float32)
    average = lax.optimization_barrier(jnp.mean(values_f, axis=-1, keepdims=True))
    centred = values_f - average
    variance = lax.optimization_barrier(jnp.mean(centred * centred, axis=-1, keepdims=True))
    return (centred * lax.rsqrt(variance + EPSILON)).astype(jnp.bfloat16)

def project_heads(columns, proj_weight, gate_bias, head_count):
    projected = jnp.einsum('cnz,zf->cnf', columns.astype(jnp.float32), proj_weight.astype(jnp.float32))
    inner_width = proj_weight.shape[1] // 4
    head_dim = inner_width // head_count
    head_shape = columns.shape[:2] + (head_count, head_dim)
    query = (projected[..., :inner_width] * head_dim ** (-0.5)).astype(jnp.bfloat16).reshape(head_shape)
    keys_all = projected[..., inner_width:2 * inner_width].astype(jnp.bfloat16).reshape(head_shape)
    values = projected[..., 2 * inner_width:3 * inner_width].astype(jnp.bfloat16).reshape(head_shape)
    gating = jax.nn.sigmoid(projected[..., 3 * inner_width:] + gate_bias.astype(jnp.float32))
    return (query, keys_all, values, gating)

def reference(pair_repr, proj_weight, gate_bias, bias_weight, out_weight, out_bias):
    residues = pair_repr.shape[0]
    channels = pair_repr.shape[2]
    head_count = bias_weight.shape[1]
    normed = normalize(pair_repr)
    pair_bias = jnp.einsum('knc,ch->hkn', normed.astype(jnp.float32), bias_weight.astype(jnp.float32))
    group_size = math.gcd(residues, 8)
    columns = jnp.transpose(normed, (1, 0, 2)).reshape(residues // group_size, group_size, residues, channels)

    def column_group(block):
        query, keys_all, values, gating = project_heads(block, proj_weight, gate_bias, head_count)
        scores = jnp.einsum('ckhd,cqhd->chkq', keys_all.astype(jnp.float32), query.astype(jnp.float32)) + pair_bias[None]
        row_max = lax.optimization_barrier(jnp.max(scores, axis=2, keepdims=True))
        expd = jnp.exp(scores - row_max)
        row_total = lax.optimization_barrier(jnp.sum(expd, axis=2))
        weights = expd.astype(jnp.bfloat16)
        attended = jnp.einsum('chkq,ckhd->cqhd', weights.astype(jnp.float32), values.astype(jnp.float32))
        attended = attended / jnp.transpose(row_total, (0, 2, 1))[..., None]
        flat = attended.reshape(block.shape[0], residues, -1)
        gated = (gating * flat).astype(jnp.bfloat16)
        update = jnp.einsum('cnf,fz->cnz', gated.astype(jnp.float32), out_weight.astype(jnp.float32))
        return (update + out_bias.astype(jnp.float32)).astype(jnp.bfloat16)
    results = lax.map(column_group, columns)
    results = results.reshape(residues, residues, channels)
    return jnp.transpose(results, (1, 0, 2))
```

```python
import functools

import jax
import jax.numpy as jnp
from jax import lax
from jax.experimental import pallas as pl
from jax.experimental.pallas import tpu as pltpu
from jax.sharding import PartitionSpec as P

EPSILON = 1e-05
MESH = pl.DeviceIdType.MESH
LANES = 128
NT = (((1,), (1,)), ((), ()))


def nt_dot(a, b):
    return lax.dot_general(a, b, NT, preferred_element_type=jnp.float32)


def exchange_kernel(
    chips,
    heads,
    x_ref,
    proj_ref,
    gate_bias_ref,
    bias_weight_ref,
    out_ref,
    xin,
    flat,
    bias_rows,
    send_buf,
    cols,
    bias,
    proj_t,
    gate_col,
    keys,
    values_t,
    result,
    send_out,
    in_local_sem,
    in_send_sem,
    in_recv_sem,
    ring_send_sem,
    ring_recv_sem,
    pair_send_sem,
    pair_recv_sem,
    a2a_send_sem,
    a2a_recv_sem,
    out_local_sem,
    out_send_sem,
    out_recv_sem,
):
    local_rows = x_ref.shape[0]
    pair_rows = 2 * local_rows
    blocks = cols.shape[2]
    spread = cols.shape[1]
    width = cols.shape[0]
    channels = x_ref.shape[4]
    half = send_buf.shape[0] * width
    row = lax.axis_index("row")
    chip = row // 2
    core = lax.rem(row, 2)
    partner = row + 1 - 2 * core
    last = chips // 2

    def at(distance):
        return lax.rem(row + 2 * distance + 2 * chips, 2 * chips)

    barrier = pltpu.get_barrier_semaphore()
    for other in (partner, at(1), at(-1)):
        pl.semaphore_signal(barrier, inc=1, device_id={"row": other}, device_id_type=MESH)

    proj_t[...] = proj_ref[...].astype(jnp.float32).T.astype(jnp.bfloat16)
    gate_col[...] = jnp.broadcast_to(gate_bias_ref[...], (channels, channels)).T
    eye = (
        lax.broadcasted_iota(jnp.int32, (8, heads), 0) == lax.broadcasted_iota(jnp.int32, (8, heads), 1)
    ).astype(jnp.float32)
    bias_w = nt_dot(eye, bias_weight_ref[...].astype(jnp.float32)).astype(jnp.bfloat16)

    keep = pltpu.make_async_copy(x_ref.at[:, :, core], xin.at[core], in_local_sem)
    keep.start()
    pl.semaphore_wait(barrier, 3)
    swap = pltpu.make_async_remote_copy(
        src_ref=x_ref.at[:, :, 1 - core],
        dst_ref=xin.at[core],
        send_sem=in_send_sem,
        recv_sem=in_recv_sem,
        device_id={"row": partner},
        device_id_type=MESH,
    )
    swap.start()
    keep.wait()
    swap.wait()

    def normalize_row(index, _):
        part = index // local_rows
        line = lax.rem(index, local_rows)
        x = xin[part, line].reshape(half, channels).astype(jnp.float32)
        centred = x - jnp.mean(x, axis=-1, keepdims=True)
        variance = jnp.mean(centred * centred, axis=-1, keepdims=True)
        normed = centred * lax.rsqrt(variance + EPSILON)
        rounded = normed.astype(jnp.bfloat16)
        groups = [rounded[g * pair_rows : (g + 1) * pair_rows] for g in range(half // pair_rows)]
        ordered = [groups[a * (blocks // 2) + block] for block in range(blocks // 2) for a in range(spread)]
        row_bias = nt_dot(bias_w, jnp.concatenate(ordered, axis=0))
        for block in range(blocks // 2):
            lanes = slice(block * LANES, (block + 1) * LANES)
            bias_rows[block, pl.ds(pl.multiple_of(index * 8, 8), 8), :] = row_bias[:, lanes]
        flat[pl.ds(index, half, stride=pair_rows), :] = normed
        return 0

    lax.fori_loop(0, pair_rows, normalize_row, 0)
    for block in range(blocks // 2):
        for h in range(heads):
            piece = bias_rows[block, pl.ds(h, pair_rows, stride=8), :]
            bias[core * (blocks // 2) + block, chip, :, h * LANES : (h + 1) * LANES] = piece

    mine = pl.ds(core * (blocks // 2), blocks // 2)

    def ring_copy(source, step, direction, target):
        ref = bias.at[mine, source]
        return pltpu.make_async_remote_copy(
            src_ref=ref,
            dst_ref=ref,
            send_sem=ring_send_sem,
            recv_sem=ring_recv_sem.at[direction, step],
            device_id={"row": target},
            device_id_type=MESH,
        )

    def pair_copy(source):
        ref = bias.at[mine, source]
        return pltpu.make_async_remote_copy(
            src_ref=ref,
            dst_ref=ref,
            send_sem=pair_send_sem,
            recv_sem=pair_recv_sem,
            device_id={"row": partner},
            device_id_type=MESH,
        )

    def column_copy(distance):
        target = at(distance)
        target_chip = target // 2
        return pltpu.make_async_remote_copy(
            src_ref=send_buf.at[target_chip],
            dst_ref=cols.at[:, chip // blocks, lax.rem(chip, blocks)],
            send_sem=a2a_send_sem,
            recv_sem=a2a_recv_sem,
            device_id={"row": target},
            device_id_type=MESH,
        )

    ring_copy(chip, 0, 0, at(1)).start()
    ring_copy(chip, 0, 1, at(-1)).start()
    pair_copy(chip).start()

    def round_chunk(index, _):
        rows = width * pair_rows
        piece = flat[pl.ds(pl.multiple_of(index * rows, rows), rows), :]
        send_buf[index] = piece.reshape(width, pair_rows, channels).astype(jnp.bfloat16)
        return 0

    lax.fori_loop(0, chips, round_chunk, 0)
    cols[:, chip // blocks, lax.rem(chip, blocks)] = send_buf[chip]

    def chip_at(distance):
        return at(distance) // 2

    def ring_step(step, _):
        behind, ahead = chip_at(-step), chip_at(step)
        ring_copy(behind, step - 1, 0, at(1)).wait_recv()
        ring_copy(behind, step, 0, at(1)).start()
        ring_copy(ahead, step - 1, 1, at(-1)).wait_recv()

        @pl.when(step < last - 1)
        def _():
            ring_copy(ahead, step, 1, at(-1)).start()

        pair_copy(behind).start()
        pair_copy(ahead).start()
        column_copy(step).start()
        column_copy(-step).start()
        return 0

    lax.fori_loop(1, last, ring_step, 0)
    opposite = chip_at(-last)
    ring_copy(opposite, last - 1, 0, at(1)).wait_recv()
    pair_copy(opposite).start()
    column_copy(last).start()

    whole = bias.at[mine]
    pltpu.make_async_copy(whole, whole, pair_recv_sem).wait()
    others = send_buf.at[pl.ds(0, chips - 1)]
    pltpu.make_async_copy(others, others, a2a_recv_sem).wait()

    inner = proj_t.shape[0] // 4
    head_dim = inner // heads
    residues = chips * pair_rows
    block_rows = spread * pair_rows

    def project(column, _):
        x = cols[column].reshape(residues, channels)
        keys[column] = nt_dot(x, proj_t[inner : 2 * inner]).astype(jnp.bfloat16)
        values_t[column] = nt_dot(proj_t[2 * inner : 3 * inner], x).astype(jnp.bfloat16)
        return 0

    lax.fori_loop(0, width, project, 0)

    head_of_row = lax.broadcasted_iota(jnp.int32, (inner, block_rows), 0) // head_dim
    group = (chip // blocks) * (2 * blocks) + core * blocks + lax.rem(chip, blocks)

    def attend(column, block):
        x = cols[column, :, block].reshape(block_rows, channels)
        query_t = nt_dot(proj_t[0:inner], x) * head_dim ** (-0.5)
        gate_t = jax.nn.sigmoid(nt_dot(proj_t[3 * inner : 4 * inner], x) + gate_col[...])
        spread_q = jnp.concatenate(
            [jnp.where(head_of_row == h, query_t, 0.0).astype(jnp.bfloat16) for h in range(heads)], axis=1
        )
        scores = jnp.dot(keys[column], spread_q, preferred_element_type=jnp.float32)
        scores = scores + bias[block].reshape(residues, heads * block_rows)
        row_max = jnp.max(scores, axis=0, keepdims=True)
        expd = jnp.exp(scores - row_max)
        row_total = jnp.sum(expd, axis=0, keepdims=True)
        summed = jnp.dot(values_t[column], expd.astype(jnp.bfloat16), preferred_element_type=jnp.float32)
        parts = []
        for h in range(heads):
            lanes = slice(h * block_rows, (h + 1) * block_rows)
            parts.append(summed[h * head_dim : (h + 1) * head_dim, lanes] / row_total[:, lanes])
        gated_t = gate_t * jnp.concatenate(parts, axis=0)
        result[pl.ds(column, block_rows, stride=width), :] = gated_t.T

    def out_copy(block, a, target_core):
        target_chip = a * blocks + block
        return pltpu.make_async_remote_copy(
            src_ref=send_out.at[block, a, target_core],
            dst_ref=out_ref.at[:, group],
            send_sem=out_send_sem,
            recv_sem=out_recv_sem,
            device_id={"row": 2 * target_chip + target_core},
            device_id_type=MESH,
        )

    def block_step(step, _):
        block = lax.rem(chip + step, blocks)

        def column_step(column, _):
            attend(column, block)
            return 0

        lax.fori_loop(0, width, column_step, 0)
        send_out[block] = (
            result[...].reshape(spread, 2, local_rows, width, channels).astype(jnp.bfloat16)
        )

        def send(index, _):
            a = index // 2
            target_core = lax.rem(index, 2)
            own = 2 * (a * blocks + block) + target_core == row

            @pl.when(jnp.logical_not(own))
            def _():
                out_copy(block, a, target_core).start()

            return 0

        lax.fori_loop(0, 2 * spread, send, 0)
        return 0

    lax.fori_loop(0, blocks, block_step, 0)
    own_copy = pltpu.make_async_copy(
        send_out.at[lax.rem(chip, blocks), chip // blocks, core], out_ref.at[:, group], out_local_sem
    )
    own_copy.start()

    ring_blocks = bias.at[mine, pl.ds(0, chips - 1)]
    pltpu.make_async_copy(ring_blocks, ring_blocks, ring_send_sem).wait()
    pltpu.make_async_copy(whole, whole, pair_send_sem).wait()
    pltpu.make_async_copy(others, others, a2a_send_sem).wait()
    own_copy.wait()
    received = out_ref.at[:, pl.ds(0, 2 * chips - 1)]
    pltpu.make_async_copy(received, received, out_send_sem).wait()
    pltpu.make_async_copy(received, received, out_recv_sem).wait()


def on_device(row_count, pair_repr, proj_weight, gate_bias, bias_weight, out_weight, out_bias):
    local_rows, residues, channels = pair_repr.shape
    heads = bias_weight.shape[1]
    inner = proj_weight.shape[1] // 4
    chips = row_count // 2
    width = residues // row_count
    pair_rows = 2 * local_rows
    blocks = residues // LANES
    spread = chips // blocks
    vmem = pl.BlockSpec(memory_space=pltpu.VMEM)
    dma = pltpu.SemaphoreType.DMA
    gathered = pl.pallas_call(
        functools.partial(exchange_kernel, chips, heads),
        out_shape=jax.ShapeDtypeStruct((local_rows, row_count, width, channels), jnp.bfloat16),
        in_specs=[pl.BlockSpec(memory_space=pl.ANY), vmem, vmem, vmem],
        out_specs=pl.BlockSpec(memory_space=pl.ANY),
        scratch_shapes=[
            pltpu.VMEM((2, local_rows, spread, residues // (2 * spread), channels), jnp.bfloat16),
            pltpu.VMEM((residues // 2 * pair_rows, channels), jnp.float32),
            pltpu.VMEM((blocks // 2, 8 * pair_rows, LANES), jnp.float32),
            pltpu.VMEM((chips, width, pair_rows, channels), jnp.bfloat16),
            pltpu.VMEM((width, spread, blocks, pair_rows, channels), jnp.bfloat16),
            pltpu.VMEM((blocks, chips, pair_rows, heads * LANES), jnp.float32),
            pltpu.VMEM((4 * inner, channels), jnp.bfloat16),
            pltpu.VMEM((channels, channels), jnp.float32),
            pltpu.VMEM((width, residues, inner), jnp.bfloat16),
            pltpu.VMEM((width, inner, residues), jnp.bfloat16),
            pltpu.VMEM((LANES * width, inner), jnp.float32),
            pltpu.VMEM((blocks, spread, 2, local_rows, width, inner), jnp.bfloat16),
            dma,
            dma,
            dma,
            dma,
            dma((2, chips // 2)),
            dma,
            dma,
            dma,
            dma,
            dma,
            dma,
            dma,
        ],
        compiler_params=pltpu.CompilerParams(collective_id=0, has_side_effects=True, vmem_limit_bytes=60 * 2**20),
    )(
        pair_repr.reshape(local_rows, spread, 2, residues // (2 * spread), channels),
        proj_weight,
        gate_bias.reshape(1, inner),
        bias_weight,
    )
    gated = gathered.reshape(local_rows, residues, inner)
    update = jnp.einsum("cnf,fz->cnz", gated, out_weight, preferred_element_type=jnp.float32)
    return (update + out_bias).astype(jnp.bfloat16)


def solution(mesh):
    return jax.shard_map(
        functools.partial(on_device, mesh.shape["row"]),
        mesh=mesh,
        in_specs=(P(("group", "row"), None, None), P(), P(), P(), P(), P()),
        out_specs=P(("group", "row"), None, None),
        check_vma=False,
    )
```

```python
import functools

import jax
import jax.numpy as jnp
from jax import lax
from jax.experimental import pallas as pl
from jax.experimental.pallas import tpu as pltpu
from jax.sharding import PartitionSpec as P

EPSILON = 1e-05
MESH = pl.DeviceIdType.MESH
LANES = 128
NT = (((1,), (1,)), ((), ()))


def nt_dot(a, b):
    return lax.dot_general(a, b, NT, preferred_element_type=jnp.float32)


def exchange_kernel(
    chips,
    heads,
    x_ref,
    proj_hbm,
    gate_bias_hbm,
    bias_weight_hbm,
    out_ref,
    proj_ref,
    gate_bias_ref,
    bias_weight_ref,
    xin,
    flat,
    bias_rows,
    send_buf,
    cols,
    bias,
    proj_t,
    gate_col,
    keys,
    values_t,
    result,
    send_out,
    weight_sems,
    in_local_sem,
    in_send_sem,
    in_recv_sem,
    ring_send_sem,
    ring_recv_sem,
    pair_send_sem,
    pair_recv_sem,
    a2a_send_sem,
    a2a_recv_sem,
    out_send_sem,
    out_recv_sem,
):
    local_rows = x_ref.shape[0]
    pair_rows = 2 * local_rows
    blocks = cols.shape[2]
    spread = cols.shape[1]
    width = cols.shape[0]
    channels = x_ref.shape[4]
    half = send_buf.shape[0] * width
    row = lax.axis_index("row")
    chip = row // 2
    core = lax.rem(row, 2)
    partner = row + 1 - 2 * core
    last = chips // 2
    first, tail = width // 2, width // 8
    chunks = ((0, first), (first, width - first - tail), (width - tail, tail))

    def at(distance):
        return lax.rem(row + 2 * distance + 2 * chips, 2 * chips)

    barrier = pltpu.get_barrier_semaphore()
    for other in (partner, at(1), at(-1)):
        pl.semaphore_signal(barrier, inc=1, device_id={"row": other}, device_id_type=MESH)
    keep = pltpu.make_async_copy(x_ref.at[:, :, core], xin.at[core], in_local_sem)
    keep.start()
    weight_copies = [
        pltpu.make_async_copy(source, target, weight_sems.at[i])
        for i, (source, target) in enumerate(
            ((proj_hbm, proj_ref), (gate_bias_hbm, gate_bias_ref), (bias_weight_hbm, bias_weight_ref))
        )
    ]
    for copy in weight_copies:
        copy.start()
    for copy in weight_copies:
        copy.wait()

    proj_t[...] = proj_ref[...].astype(jnp.float32).T.astype(jnp.bfloat16)
    gate_col[...] = jnp.broadcast_to(gate_bias_ref[...], (channels, channels)).T
    bias_w = bias_weight_ref[...].astype(jnp.float32)
    bias_w = jnp.concatenate([bias_w, jnp.zeros((8 - heads, channels), jnp.float32)], axis=0).astype(jnp.bfloat16)

    pl.semaphore_wait(barrier, 3)
    swap = pltpu.make_async_remote_copy(
        src_ref=x_ref.at[:, :, 1 - core],
        dst_ref=xin.at[core],
        send_sem=in_send_sem,
        recv_sem=in_recv_sem,
        device_id={"row": partner},
        device_id_type=MESH,
    )
    swap.start()
    keep.wait()

    def normalize_row(part, line):
        index = part * local_rows + line
        x = xin[part, line].reshape(half, channels).astype(jnp.float32)
        centred = x - jnp.mean(x, axis=-1, keepdims=True)
        variance = jnp.mean(centred * centred, axis=-1, keepdims=True)
        normed = centred * lax.rsqrt(variance + EPSILON)
        rounded = normed.astype(jnp.bfloat16)
        groups = [rounded[g * pair_rows : (g + 1) * pair_rows] for g in range(half // pair_rows)]
        ordered = [groups[a * (blocks // 2) + block] for block in range(blocks // 2) for a in range(spread)]
        row_bias = nt_dot(bias_w, jnp.concatenate(ordered, axis=0))
        for block in range(blocks // 2):
            lanes = slice(block * LANES, (block + 1) * LANES)
            bias_rows[block, pl.ds(pl.multiple_of(index * 8, 8), 8), :] = row_bias[:, lanes]
        flat[pl.ds(index, half, stride=pair_rows), :] = normed

    def own_row(line, _):
        normalize_row(core, line)
        return 0

    def other_row(line, _):
        normalize_row(1 - core, line)
        return 0

    lax.fori_loop(0, local_rows, own_row, 0)
    swap.wait()
    lax.fori_loop(0, local_rows, other_row, 0)
    for block in range(blocks // 2):
        for h in range(heads):
            piece = bias_rows[block, pl.ds(h, pair_rows, stride=8), :]
            bias[core * (blocks // 2) + block, chip, :, h * LANES : (h + 1) * LANES] = piece

    mine = pl.ds(core * (blocks // 2), blocks // 2)

    def ring_copy(source, step, direction, target):
        ref = bias.at[mine, source]
        return pltpu.make_async_remote_copy(
            src_ref=ref,
            dst_ref=ref,
            send_sem=ring_send_sem,
            recv_sem=ring_recv_sem.at[direction, step],
            device_id={"row": target},
            device_id_type=MESH,
        )

    def pair_copy(source):
        ref = bias.at[mine, source]
        return pltpu.make_async_remote_copy(
            src_ref=ref,
            dst_ref=ref,
            send_sem=pair_send_sem,
            recv_sem=pair_recv_sem,
            device_id={"row": partner},
            device_id_type=MESH,
        )

    def column_copy(distance, chunk):
        target = at(distance)
        part = pl.ds(*chunks[chunk])
        return pltpu.make_async_remote_copy(
            src_ref=send_buf.at[target // 2, part],
            dst_ref=cols.at[part, chip // blocks, lax.rem(chip, blocks)],
            send_sem=a2a_send_sem,
            recv_sem=a2a_recv_sem.at[chunk],
            device_id={"row": target},
            device_id_type=MESH,
        )

    ring_copy(chip, 0, 0, at(1)).start()
    ring_copy(chip, 0, 1, at(-1)).start()
    pair_copy(chip).start()

    def round_chunk(index, _):
        rows = width * pair_rows
        piece = flat[pl.ds(pl.multiple_of(index * rows, rows), rows), :]
        send_buf[index] = piece.reshape(width, pair_rows, channels).astype(jnp.bfloat16)
        return 0

    lax.fori_loop(0, chips, round_chunk, 0)
    cols[:, chip // blocks, lax.rem(chip, blocks)] = send_buf[chip]

    def chip_at(distance):
        return at(distance) // 2

    def ring_step(step, _):
        behind, ahead = chip_at(-step), chip_at(step)
        ring_copy(behind, step - 1, 0, at(1)).wait_recv()
        ring_copy(behind, step, 0, at(1)).start()
        ring_copy(ahead, step - 1, 1, at(-1)).wait_recv()

        @pl.when(step < last - 1)
        def _():
            ring_copy(ahead, step, 1, at(-1)).start()

        pair_copy(behind).start()
        pair_copy(ahead).start()
        column_copy(step, 0).start()
        column_copy(-step, 0).start()
        return 0

    lax.fori_loop(1, last, ring_step, 0)
    opposite = chip_at(-last)
    ring_copy(opposite, last - 1, 0, at(1)).wait_recv()
    pair_copy(opposite).start()
    column_copy(last, 0).start()
    for chunk in range(1, len(chunks)):
        column_copy(last, chunk).start()

        def send_columns(nearer, _, chunk=chunk):
            column_copy(last - nearer, chunk).start()
            column_copy(nearer - last, chunk).start()
            return 0

        lax.fori_loop(1, last, send_columns, 0)

    whole = bias.at[mine]
    others = send_buf.at[pl.ds(0, chips - 1)]

    inner = proj_t.shape[0] // 4
    head_dim = inner // heads
    residues = chips * pair_rows
    block_rows = spread * pair_rows

    def project(column, _):
        x = cols[column].reshape(residues, channels)
        keys[column] = nt_dot(x, proj_t[inner : 2 * inner]).astype(jnp.bfloat16)
        values_t[column] = nt_dot(proj_t[2 * inner : 3 * inner], x).astype(jnp.bfloat16)
        return 0

    head_of_row = lax.broadcasted_iota(jnp.int32, (inner, block_rows), 0) // head_dim
    group = (chip // blocks) * (2 * blocks) + core * blocks + lax.rem(chip, blocks)

    def attend(column, block):
        x = cols[column, :, block].reshape(block_rows, channels)
        query_t = nt_dot(proj_t[0:inner], x) * head_dim ** (-0.5)
        gate_t = jax.nn.sigmoid(nt_dot(proj_t[3 * inner : 4 * inner], x) + gate_col[...])
        spread_q = jnp.concatenate(
            [jnp.where(head_of_row == h, query_t, 0.0).astype(jnp.bfloat16) for h in range(heads)], axis=1
        )
        scores = jnp.dot(keys[column], spread_q, preferred_element_type=jnp.float32)
        scores = scores + bias[block].reshape(residues, heads * block_rows)
        row_max = jnp.max(scores, axis=0, keepdims=True)
        expd = jnp.exp(scores - row_max)
        row_total = jnp.sum(expd, axis=0, keepdims=True)
        summed = jnp.dot(values_t[column], expd.astype(jnp.bfloat16), preferred_element_type=jnp.float32)
        parts = []
        for h in range(heads):
            lanes = slice(h * block_rows, (h + 1) * block_rows)
            parts.append(summed[h * head_dim : (h + 1) * head_dim, lanes] / row_total[:, lanes])
        gated_t = gate_t * jnp.concatenate(parts, axis=0)
        result[block, pl.ds(column, block_rows, stride=width), :] = gated_t.T

    def out_copy(block, a, target_core):
        target_chip = a * blocks + block
        return pltpu.make_async_remote_copy(
            src_ref=send_out.at[block, a, target_core],
            dst_ref=out_ref.at[:, group],
            send_sem=out_send_sem,
            recv_sem=out_recv_sem,
            device_id={"row": 2 * target_chip + target_core},
            device_id_type=MESH,
        )

    def attend_block(step, chunk):
        block = lax.rem(chip + step, blocks)
        start, count = chunks[chunk]

        def column_step(column, _):
            attend(column, block)
            return 0

        lax.fori_loop(start, start + count, column_step, 0)
        return block

    def send_block(step, _):
        block = attend_block(step, len(chunks) - 1)
        send_out[block] = result[block].reshape(spread, 2, local_rows, width, channels).astype(jnp.bfloat16)

        def send(index, _):
            order = index // 2
            jump = spread // 2 + (order // 2 + lax.rem(order, 2)) * (1 - 2 * lax.rem(order, 2))
            target_chip = lax.rem(chip + step + blocks * jump, chips)
            target_core = lax.rem(core + index, 2)

            @pl.when(2 * target_chip + target_core != row)
            def _():
                out_copy(block, target_chip // blocks, target_core).start()

            return 0

        lax.fori_loop(0, 2 * spread, send, 0)
        return 0

    pltpu.make_async_copy(whole, whole, pair_recv_sem).wait()
    for chunk, (start, count) in enumerate(chunks):
        arrived = send_buf.at[pl.ds(0, chips - 1), pl.ds(0, count)]
        pltpu.make_async_copy(arrived, arrived, a2a_recv_sem.at[chunk]).wait()
        lax.fori_loop(start, start + count, project, 0)
        if chunk < len(chunks) - 1:

            def attend_early(step, _, chunk=chunk):
                attend_block(step, chunk)
                return 0

            lax.fori_loop(0, blocks, attend_early, 0)
    lax.fori_loop(0, blocks, send_block, 0)
    out_ref[:, group] = send_out[lax.rem(chip, blocks), chip // blocks, core]

    ring_blocks = bias.at[mine, pl.ds(0, chips - 1)]
    pltpu.make_async_copy(ring_blocks, ring_blocks, ring_send_sem).wait()
    pltpu.make_async_copy(whole, whole, pair_send_sem).wait()
    pltpu.make_async_copy(others, others, a2a_send_sem).wait()
    received = out_ref.at[:, pl.ds(0, 2 * chips - 1)]
    pltpu.make_async_copy(received, received, out_send_sem).wait()
    pltpu.make_async_copy(received, received, out_recv_sem).wait()


def on_device(row_count, pair_repr, proj_weight, gate_bias, bias_weight, out_weight, out_bias):
    local_rows, residues, channels = pair_repr.shape
    heads = bias_weight.shape[1]
    inner = proj_weight.shape[1] // 4
    chips = row_count // 2
    width = residues // row_count
    pair_rows = 2 * local_rows
    blocks = residues // LANES
    spread = chips // blocks
    dma = pltpu.SemaphoreType.DMA
    gathered = pl.pallas_call(
        functools.partial(exchange_kernel, chips, heads),
        out_shape=jax.ShapeDtypeStruct((local_rows, row_count, width, channels), jnp.bfloat16),
        in_specs=[pl.BlockSpec(memory_space=pltpu.HBM)] * 4,
        out_specs=pl.BlockSpec(memory_space=pltpu.VMEM),
        scratch_shapes=[
            pltpu.VMEM((channels, 4 * inner), jnp.bfloat16),
            pltpu.VMEM((1, inner), jnp.float32),
            pltpu.VMEM((heads, channels), jnp.bfloat16),
            pltpu.VMEM((2, local_rows, spread, residues // (2 * spread), channels), jnp.bfloat16),
            pltpu.VMEM((residues // 2 * pair_rows, channels), jnp.float32),
            pltpu.VMEM((blocks // 2, 8 * pair_rows, LANES), jnp.float32),
            pltpu.VMEM((chips, width, pair_rows, channels), jnp.bfloat16),
            pltpu.VMEM((width, spread, blocks, pair_rows, channels), jnp.bfloat16),
            pltpu.VMEM((blocks, chips, pair_rows, heads * LANES), jnp.float32),
            pltpu.VMEM((4 * inner, channels), jnp.bfloat16),
            pltpu.VMEM((channels, channels), jnp.float32),
            pltpu.VMEM((width, residues, inner), jnp.bfloat16),
            pltpu.VMEM((width, inner, residues), jnp.bfloat16),
            pltpu.VMEM((blocks, LANES * width, inner), jnp.float32),
            pltpu.VMEM((blocks, spread, 2, local_rows, width, inner), jnp.bfloat16),
            dma((3,)),
            dma,
            dma,
            dma,
            dma,
            dma((2, chips // 2)),
            dma,
            dma,
            dma,
            dma((3,)),
            dma,
            dma,
        ],
        compiler_params=pltpu.CompilerParams(collective_id=0, has_side_effects=True, vmem_limit_bytes=28 * 2**20),
    )(
        *(
            pltpu.with_memory_space_constraint(array, pltpu.HBM)
            for array in (
                pair_repr.reshape(local_rows, spread, 2, residues // (2 * spread), channels),
                proj_weight,
                gate_bias.reshape(1, inner),
                bias_weight.T,
            )
        )
    )
    gated = gathered.reshape(local_rows, residues, inner)
    update = jnp.einsum("cnf,fz->cnz", gated, out_weight, preferred_element_type=jnp.float32)
    return (update + out_bias).astype(jnp.bfloat16)


def solution(mesh):
    return jax.shard_map(
        functools.partial(on_device, mesh.shape["row"]),
        mesh=mesh,
        in_specs=(P(("group", "row"), None, None), P(), P(), P(), P(), P()),
        out_specs=P(("group", "row"), None, None),
        check_vma=False,
    )
```

```python
import functools

import jax
import jax.numpy as jnp
from jax import lax
from jax.experimental import pallas as pl
from jax.experimental.pallas import tpu as pltpu
from jax.sharding import PartitionSpec as P

EPSILON = 1e-05
MESH = pl.DeviceIdType.MESH
LANES = 128
NT = (((1,), (1,)), ((), ()))


def nt_dot(a, b):
    return lax.dot_general(a, b, NT, preferred_element_type=jnp.float32)


def exchange_kernel(
    chips,
    heads,
    x_ref,
    proj_hbm,
    gate_bias_hbm,
    bias_weight_hbm,
    out_ref,
    proj_ref,
    gate_bias_ref,
    bias_weight_ref,
    xin,
    flat,
    bias_rows,
    send_buf,
    cols,
    bias,
    proj_t,
    gate_col,
    keys,
    values_t,
    send_out,
    weight_sems,
    in_local_sem,
    in_send_sem,
    in_recv_sem,
    ring_send_sem,
    ring_recv_sem,
    pair_send_sem,
    pair_recv_sem,
    a2a_send_sem,
    a2a_recv_sem,
    out_send_sem,
    out_recv_sem,
):
    local_rows = x_ref.shape[0]
    pair_rows = 2 * local_rows
    blocks = cols.shape[2]
    spread = cols.shape[1]
    width = cols.shape[0]
    channels = x_ref.shape[4]
    half = send_buf.shape[0] * width
    row = lax.axis_index("row")
    chip = row // 2
    core = lax.rem(row, 2)
    partner = row + 1 - 2 * core
    last = chips // 2
    first = width // 2
    chunks = ((0, first), (first, width - first))

    def at(distance):
        return lax.rem(row + 2 * distance + 2 * chips, 2 * chips)

    barrier = pltpu.get_barrier_semaphore()
    for other in (partner, at(1), at(-1)):
        pl.semaphore_signal(barrier, inc=1, device_id={"row": other}, device_id_type=MESH)
    keep = pltpu.make_async_copy(x_ref.at[:, :, core], xin.at[core], in_local_sem)
    keep.start()
    weight_copies = [
        pltpu.make_async_copy(source, target, weight_sems.at[i])
        for i, (source, target) in enumerate(
            ((proj_hbm, proj_ref), (gate_bias_hbm, gate_bias_ref), (bias_weight_hbm, bias_weight_ref))
        )
    ]
    for copy in weight_copies:
        copy.start()
    for copy in weight_copies:
        copy.wait()

    proj_t[...] = proj_ref[...].astype(jnp.float32).T.astype(jnp.bfloat16)
    gate_col[...] = jnp.broadcast_to(gate_bias_ref[...], (channels, channels)).T
    bias_w = bias_weight_ref[...].astype(jnp.float32)
    bias_w = jnp.concatenate([bias_w, jnp.zeros((8 - heads, channels), jnp.float32)], axis=0).astype(jnp.bfloat16)

    pl.semaphore_wait(barrier, 3)
    swap = pltpu.make_async_remote_copy(
        src_ref=x_ref.at[:, :, 1 - core],
        dst_ref=xin.at[core],
        send_sem=in_send_sem,
        recv_sem=in_recv_sem,
        device_id={"row": partner},
        device_id_type=MESH,
    )
    swap.start()
    keep.wait()

    def normalize_row(part, line):
        index = part * local_rows + line
        x = xin[part, line].reshape(half, channels).astype(jnp.float32)
        centred = x - jnp.mean(x, axis=-1, keepdims=True)
        variance = jnp.mean(centred * centred, axis=-1, keepdims=True)
        normed = centred * lax.rsqrt(variance + EPSILON)
        rounded = normed.astype(jnp.bfloat16)
        groups = [rounded[g * pair_rows : (g + 1) * pair_rows] for g in range(half // pair_rows)]
        ordered = [groups[a * (blocks // 2) + block] for block in range(blocks // 2) for a in range(spread)]
        row_bias = nt_dot(bias_w, jnp.concatenate(ordered, axis=0))
        for block in range(blocks // 2):
            lanes = slice(block * LANES, (block + 1) * LANES)
            bias_rows[block, pl.ds(pl.multiple_of(index * 8, 8), 8), :] = row_bias[:, lanes]
        flat[pl.ds(index, half, stride=pair_rows), :] = normed

    def own_row(line, _):
        normalize_row(core, line)
        return 0

    def other_row(line, _):
        normalize_row(1 - core, line)
        return 0

    lax.fori_loop(0, local_rows, own_row, 0)
    swap.wait()
    lax.fori_loop(0, local_rows, other_row, 0)
    for block in range(blocks // 2):
        for h in range(heads):
            piece = bias_rows[block, pl.ds(h, pair_rows, stride=8), :]
            bias[core * (blocks // 2) + block, chip, :, h * LANES : (h + 1) * LANES] = piece

    mine = pl.ds(core * (blocks // 2), blocks // 2)

    def ring_copy(source, step, direction, target):
        ref = bias.at[mine, source]
        return pltpu.make_async_remote_copy(
            src_ref=ref,
            dst_ref=ref,
            send_sem=ring_send_sem,
            recv_sem=ring_recv_sem.at[direction, step],
            device_id={"row": target},
            device_id_type=MESH,
        )

    def pair_copy(source):
        ref = bias.at[mine, source]
        return pltpu.make_async_remote_copy(
            src_ref=ref,
            dst_ref=ref,
            send_sem=pair_send_sem,
            recv_sem=pair_recv_sem,
            device_id={"row": partner},
            device_id_type=MESH,
        )

    def column_copy(distance, chunk):
        target = at(distance)
        part = pl.ds(*chunks[chunk])
        return pltpu.make_async_remote_copy(
            src_ref=send_buf.at[target // 2, part],
            dst_ref=cols.at[part, chip // blocks, lax.rem(chip, blocks)],
            send_sem=a2a_send_sem,
            recv_sem=a2a_recv_sem.at[chunk],
            device_id={"row": target},
            device_id_type=MESH,
        )

    ring_copy(chip, 0, 0, at(1)).start()
    ring_copy(chip, 0, 1, at(-1)).start()
    pair_copy(chip).start()

    def round_chunk(index, _):
        rows = width * pair_rows
        piece = flat[pl.ds(pl.multiple_of(index * rows, rows), rows), :]
        send_buf[index] = piece.reshape(width, pair_rows, channels).astype(jnp.bfloat16)
        return 0

    lax.fori_loop(0, chips, round_chunk, 0)
    cols[:, chip // blocks, lax.rem(chip, blocks)] = send_buf[chip]

    def chip_at(distance):
        return at(distance) // 2

    def ring_step(step, _):
        behind, ahead = chip_at(-step), chip_at(step)
        ring_copy(behind, step - 1, 0, at(1)).wait_recv()
        ring_copy(behind, step, 0, at(1)).start()
        ring_copy(ahead, step - 1, 1, at(-1)).wait_recv()

        @pl.when(step < last - 1)
        def _():
            ring_copy(ahead, step, 1, at(-1)).start()

        pair_copy(behind).start()
        pair_copy(ahead).start()
        column_copy(step, 0).start()
        column_copy(-step, 0).start()
        return 0

    lax.fori_loop(1, last, ring_step, 0)
    opposite = chip_at(-last)
    ring_copy(opposite, last - 1, 0, at(1)).wait_recv()
    pair_copy(opposite).start()
    column_copy(last, 0).start()
    for chunk in range(1, len(chunks)):
        column_copy(last, chunk).start()

        def send_columns(nearer, _, chunk=chunk):
            column_copy(last - nearer, chunk).start()
            column_copy(nearer - last, chunk).start()
            return 0

        lax.fori_loop(1, last, send_columns, 0)

    whole = bias.at[mine]
    others = send_buf.at[pl.ds(0, chips - 1)]

    inner = proj_t.shape[0] // 4
    head_dim = inner // heads
    residues = chips * pair_rows
    block_rows = spread * pair_rows

    def project(column, _):
        x = cols[column].reshape(residues, channels)
        keys[column] = nt_dot(x, proj_t[inner : 2 * inner]).astype(jnp.bfloat16)
        values_t[column] = nt_dot(proj_t[2 * inner : 3 * inner], x).astype(jnp.bfloat16)
        return 0

    head_of_row = lax.broadcasted_iota(jnp.int32, (inner, block_rows), 0) // head_dim
    group = (chip // blocks) * (2 * blocks) + core * blocks + lax.rem(chip, blocks)

    def attend(column, block):
        x = cols[column, :, block].reshape(block_rows, channels)
        query_t = nt_dot(proj_t[0:inner], x) * head_dim ** (-0.5)
        gate_t = jax.nn.sigmoid(nt_dot(proj_t[3 * inner : 4 * inner], x) + gate_col[...])
        spread_q = jnp.concatenate(
            [jnp.where(head_of_row == h, query_t, 0.0).astype(jnp.bfloat16) for h in range(heads)], axis=1
        )
        scores = jnp.dot(keys[column], spread_q, preferred_element_type=jnp.float32)
        scores = scores + bias[block].reshape(residues, heads * block_rows)
        row_max = jnp.max(scores, axis=0, keepdims=True)
        expd = jnp.exp(scores - row_max)
        row_total = jnp.sum(expd, axis=0, keepdims=True)
        summed = jnp.dot(values_t[column], expd.astype(jnp.bfloat16), preferred_element_type=jnp.float32)
        parts = []
        for h in range(heads):
            lanes = slice(h * block_rows, (h + 1) * block_rows)
            parts.append(summed[h * head_dim : (h + 1) * head_dim, lanes] / row_total[:, lanes])
        gated_t = gate_t * jnp.concatenate(parts, axis=0)
        rows = gated_t.T.reshape(spread, 2, local_rows, channels)
        send_out[block, :, :, column] = rows.astype(jnp.bfloat16)

    def out_copy(block, a, target_core, chunk):
        part = pl.ds(*chunks[chunk])
        return pltpu.make_async_remote_copy(
            src_ref=send_out.at[block, a, target_core, part],
            dst_ref=out_ref.at[group, part],
            send_sem=out_send_sem,
            recv_sem=out_recv_sem,
            device_id={"row": 2 * (a * blocks + block) + target_core},
            device_id_type=MESH,
        )

    def block_step(step, chunk):
        block = lax.rem(chip + step, blocks)
        start, count = chunks[chunk]

        def column_step(column, _):
            attend(column, block)
            return 0

        lax.fori_loop(start, start + count, column_step, 0)

        def send(index, _):
            order = index // 2
            jump = spread // 2 + (order // 2 + lax.rem(order, 2)) * (1 - 2 * lax.rem(order, 2))
            target_chip = lax.rem(chip + step + blocks * jump, chips)
            target_core = lax.rem(core + index, 2)

            @pl.when(2 * target_chip + target_core != row)
            def _():
                out_copy(block, target_chip // blocks, target_core, chunk).start()

            return 0

        lax.fori_loop(0, 2 * spread, send, 0)

    pltpu.make_async_copy(whole, whole, pair_recv_sem).wait()
    for chunk, (start, count) in enumerate(chunks):
        arrived = send_buf.at[pl.ds(0, chips - 1), pl.ds(0, count)]
        pltpu.make_async_copy(arrived, arrived, a2a_recv_sem.at[chunk]).wait()
        lax.fori_loop(start, start + count, project, 0)

        def chunk_step(step, _, chunk=chunk):
            block_step(step, chunk)
            return 0

        lax.fori_loop(0, blocks, chunk_step, 0)
    out_ref[group] = send_out[lax.rem(chip, blocks), chip // blocks, core]

    ring_blocks = bias.at[mine, pl.ds(0, chips - 1)]
    pltpu.make_async_copy(ring_blocks, ring_blocks, ring_send_sem).wait()
    pltpu.make_async_copy(whole, whole, pair_send_sem).wait()
    pltpu.make_async_copy(others, others, a2a_send_sem).wait()
    received = out_ref.at[pl.ds(0, 2 * chips - 1)]
    pltpu.make_async_copy(received, received, out_send_sem).wait()
    pltpu.make_async_copy(received, received, out_recv_sem).wait()


def on_device(row_count, pair_repr, proj_weight, gate_bias, bias_weight, out_weight, out_bias):
    local_rows, residues, channels = pair_repr.shape
    heads = bias_weight.shape[1]
    inner = proj_weight.shape[1] // 4
    chips = row_count // 2
    width = residues // row_count
    pair_rows = 2 * local_rows
    blocks = residues // LANES
    spread = chips // blocks
    dma = pltpu.SemaphoreType.DMA
    gathered = pl.pallas_call(
        functools.partial(exchange_kernel, chips, heads),
        out_shape=jax.ShapeDtypeStruct((row_count, width, local_rows, channels), jnp.bfloat16),
        in_specs=[pl.BlockSpec(memory_space=pltpu.HBM)] * 4,
        out_specs=pl.BlockSpec(memory_space=pltpu.VMEM),
        scratch_shapes=[
            pltpu.VMEM((channels, 4 * inner), jnp.bfloat16),
            pltpu.VMEM((1, inner), jnp.float32),
            pltpu.VMEM((heads, channels), jnp.bfloat16),
            pltpu.VMEM((2, local_rows, spread, residues // (2 * spread), channels), jnp.bfloat16),
            pltpu.VMEM((residues // 2 * pair_rows, channels), jnp.float32),
            pltpu.VMEM((blocks // 2, 8 * pair_rows, LANES), jnp.float32),
            pltpu.VMEM((chips, width, pair_rows, channels), jnp.bfloat16),
            pltpu.VMEM((width, spread, blocks, pair_rows, channels), jnp.bfloat16),
            pltpu.VMEM((blocks, chips, pair_rows, heads * LANES), jnp.float32),
            pltpu.VMEM((4 * inner, channels), jnp.bfloat16),
            pltpu.VMEM((channels, channels), jnp.float32),
            pltpu.VMEM((width, residues, inner), jnp.bfloat16),
            pltpu.VMEM((width, inner, residues), jnp.bfloat16),
            pltpu.VMEM((blocks, spread, 2, width, local_rows, inner), jnp.bfloat16),
            dma((3,)),
            dma,
            dma,
            dma,
            dma,
            dma((2, chips // 2)),
            dma,
            dma,
            dma,
            dma((2,)),
            dma,
            dma,
        ],
        compiler_params=pltpu.CompilerParams(collective_id=0, has_side_effects=True, vmem_limit_bytes=28 * 2**20),
    )(
        *(
            pltpu.with_memory_space_constraint(array, pltpu.HBM)
            for array in (
                pair_repr.reshape(local_rows, spread, 2, residues // (2 * spread), channels),
                proj_weight,
                gate_bias.reshape(1, inner),
                bias_weight.T,
            )
        )
    )
    gated = gathered.reshape(residues, local_rows, inner)
    update = jnp.einsum("ncf,fz->cnz", gated, out_weight, preferred_element_type=jnp.float32)
    return (update + out_bias).astype(jnp.bfloat16)


def solution(mesh):
    return jax.shard_map(
        functools.partial(on_device, mesh.shape["row"]),
        mesh=mesh,
        in_specs=(P(("group", "row"), None, None), P(), P(), P(), P(), P()),
        out_specs=P(("group", "row"), None, None),
        check_vma=False,
    )
```

```python
import functools

import jax
import jax.numpy as jnp
from jax import lax
from jax.experimental import pallas as pl
from jax.experimental.pallas import tpu as pltpu
from jax.sharding import PartitionSpec as P

EPSILON = 1e-05
MESH = pl.DeviceIdType.MESH
LANES = 128
NT = (((1,), (1,)), ((), ()))


def nt_dot(a, b):
    return lax.dot_general(a, b, NT, preferred_element_type=jnp.float32)


def exchange_kernel(
    chips,
    heads,
    x_ref,
    proj_hbm,
    gate_bias_hbm,
    bias_weight_hbm,
    out_ref,
    proj_ref,
    gate_bias_ref,
    bias_weight_ref,
    xin,
    flat,
    bias_rows,
    send_buf,
    cols,
    bias,
    proj_t,
    gate_col,
    keys,
    values_t,
    send_out,
    weight_sems,
    in_local_sem,
    in_send_sem,
    in_recv_sem,
    ring_send_sem,
    ring_recv_sem,
    pair_send_sem,
    pair_recv_sem,
    a2a_send_sem,
    a2a_recv_sem,
    out_send_sem,
    out_recv_sem,
):
    local_rows = x_ref.shape[0]
    pair_rows = 2 * local_rows
    blocks = cols.shape[2]
    spread = cols.shape[1]
    width = cols.shape[0]
    channels = x_ref.shape[4]
    half = send_buf.shape[0] * width
    row = lax.axis_index("row")
    chip = row // 2
    core = lax.rem(row, 2)
    partner = row + 1 - 2 * core
    last = chips // 2
    first = 3 * width // 4
    chunks = ((0, first), (first, width - first))

    def at(distance):
        return lax.rem(row + 2 * distance + 2 * chips, 2 * chips)

    barrier = pltpu.get_barrier_semaphore()
    for other in (partner, at(1), at(-1)):
        pl.semaphore_signal(barrier, inc=1, device_id={"row": other}, device_id_type=MESH)
    keep = pltpu.make_async_copy(x_ref.at[:, :, core], xin.at[core], in_local_sem)
    keep.start()
    weight_copies = [
        pltpu.make_async_copy(source, target, weight_sems.at[i])
        for i, (source, target) in enumerate(
            ((proj_hbm, proj_ref), (gate_bias_hbm, gate_bias_ref), (bias_weight_hbm, bias_weight_ref))
        )
    ]
    for copy in weight_copies:
        copy.start()
    pl.semaphore_wait(barrier, 3)
    swap = pltpu.make_async_remote_copy(
        src_ref=x_ref.at[:, :, 1 - core],
        dst_ref=xin.at[core],
        send_sem=in_send_sem,
        recv_sem=in_recv_sem,
        device_id={"row": partner},
        device_id_type=MESH,
    )
    swap.start()
    for copy in weight_copies:
        copy.wait()

    proj_t[...] = proj_ref[...].astype(jnp.float32).T.astype(jnp.bfloat16)
    gate_col[...] = jnp.broadcast_to(gate_bias_ref[...], (channels, channels)).T
    bias_w = bias_weight_ref[...].astype(jnp.float32)
    bias_w = jnp.concatenate([bias_w, jnp.zeros((8 - heads, channels), jnp.float32)], axis=0).astype(jnp.bfloat16)

    keep.wait()

    def normalize_row(part, line):
        index = part * local_rows + line
        x = xin[part, line].reshape(half, channels).astype(jnp.float32)
        centred = x - jnp.mean(x, axis=-1, keepdims=True)
        variance = jnp.mean(centred * centred, axis=-1, keepdims=True)
        normed = centred * lax.rsqrt(variance + EPSILON)
        rounded = normed.astype(jnp.bfloat16)
        groups = [rounded[g * pair_rows : (g + 1) * pair_rows] for g in range(half // pair_rows)]
        ordered = [groups[a * (blocks // 2) + block] for block in range(blocks // 2) for a in range(spread)]
        row_bias = nt_dot(bias_w, jnp.concatenate(ordered, axis=0))
        for block in range(blocks // 2):
            lanes = slice(block * LANES, (block + 1) * LANES)
            bias_rows[block, pl.ds(pl.multiple_of(index * 8, 8), 8), :] = row_bias[:, lanes]
        flat[pl.ds(index, half, stride=pair_rows), :] = normed

    def own_row(line, _):
        normalize_row(core, line)
        return 0

    def other_row(line, _):
        normalize_row(1 - core, line)
        return 0

    lax.fori_loop(0, local_rows, own_row, 0)
    swap.wait()
    lax.fori_loop(0, local_rows, other_row, 0)
    for block in range(blocks // 2):
        for h in range(heads):
            piece = bias_rows[block, pl.ds(h, pair_rows, stride=8), :]
            bias[core * (blocks // 2) + block, chip, :, h * LANES : (h + 1) * LANES] = piece

    mine = pl.ds(core * (blocks // 2), blocks // 2)

    def ring_copy(source, step, direction, target):
        ref = bias.at[mine, source]
        return pltpu.make_async_remote_copy(
            src_ref=ref,
            dst_ref=ref,
            send_sem=ring_send_sem,
            recv_sem=ring_recv_sem.at[direction, step],
            device_id={"row": target},
            device_id_type=MESH,
        )

    def pair_copy(source):
        ref = bias.at[mine, source]
        return pltpu.make_async_remote_copy(
            src_ref=ref,
            dst_ref=ref,
            send_sem=pair_send_sem,
            recv_sem=pair_recv_sem,
            device_id={"row": partner},
            device_id_type=MESH,
        )

    def column_copy(distance, chunk):
        target = at(distance)
        part = pl.ds(*chunks[chunk])
        return pltpu.make_async_remote_copy(
            src_ref=send_buf.at[target // 2, part],
            dst_ref=cols.at[part, chip // blocks, lax.rem(chip, blocks)],
            send_sem=a2a_send_sem,
            recv_sem=a2a_recv_sem.at[chunk],
            device_id={"row": target},
            device_id_type=MESH,
        )

    ring_copy(chip, 0, 0, at(1)).start()
    ring_copy(chip, 0, 1, at(-1)).start()
    pair_copy(chip).start()

    def round_chunk(index, _):
        rows = width * pair_rows
        piece = flat[pl.ds(pl.multiple_of(index * rows, rows), rows), :]
        send_buf[index] = piece.reshape(width, pair_rows, channels).astype(jnp.bfloat16)
        return 0

    lax.fori_loop(0, chips, round_chunk, 0)
    column_copy(1, 0).start()
    column_copy(-1, 0).start()
    cols[:, chip // blocks, lax.rem(chip, blocks)] = send_buf[chip]

    def chip_at(distance):
        return at(distance) // 2

    def ring_step(step, _):
        behind, ahead = chip_at(-step), chip_at(step)
        ring_copy(behind, step - 1, 0, at(1)).wait_recv()
        ring_copy(behind, step, 0, at(1)).start()
        ring_copy(ahead, step - 1, 1, at(-1)).wait_recv()

        @pl.when(step < last - 1)
        def _():
            ring_copy(ahead, step, 1, at(-1)).start()

        pair_copy(behind).start()
        pair_copy(ahead).start()
        column_copy(step + 1, 0).start()

        @pl.when(step + 1 < last)
        def _():
            column_copy(-step - 1, 0).start()

        return 0

    lax.fori_loop(1, last, ring_step, 0)
    opposite = chip_at(-last)
    ring_copy(opposite, last - 1, 0, at(1)).wait_recv()
    pair_copy(opposite).start()
    for chunk in range(1, len(chunks)):
        column_copy(last, chunk).start()

        def send_columns(nearer, _, chunk=chunk):
            column_copy(last - nearer, chunk).start()
            column_copy(nearer - last, chunk).start()
            return 0

        lax.fori_loop(1, last, send_columns, 0)

    whole = bias.at[mine]
    others = send_buf.at[pl.ds(0, chips - 1)]

    inner = proj_t.shape[0] // 4
    head_dim = inner // heads
    residues = chips * pair_rows
    block_rows = spread * pair_rows

    def project(column, _):
        x = cols[column].reshape(residues, channels)
        keys[column] = nt_dot(x, proj_t[inner : 2 * inner]).astype(jnp.bfloat16)
        values_t[column] = nt_dot(proj_t[2 * inner : 3 * inner], x).astype(jnp.bfloat16)
        return 0

    head_of_row = lax.broadcasted_iota(jnp.int32, (inner, block_rows), 0) // head_dim
    group = (chip // blocks) * (2 * blocks) + core * blocks + lax.rem(chip, blocks)

    def attend(column, block):
        x = cols[column, :, block].reshape(block_rows, channels)
        query_t = nt_dot(proj_t[0:inner], x) * head_dim ** (-0.5)
        gate_t = jax.nn.sigmoid(nt_dot(proj_t[3 * inner : 4 * inner], x) + gate_col[...])
        spread_q = jnp.concatenate(
            [jnp.where(head_of_row == h, query_t, 0.0).astype(jnp.bfloat16) for h in range(heads)], axis=1
        )
        scores = jnp.dot(keys[column], spread_q, preferred_element_type=jnp.float32)
        scores = scores + bias[block].reshape(residues, heads * block_rows)
        row_max = jnp.max(scores, axis=0, keepdims=True)
        expd = jnp.exp(scores - row_max)
        row_total = jnp.sum(expd, axis=0, keepdims=True)
        summed = jnp.dot(values_t[column], expd.astype(jnp.bfloat16), preferred_element_type=jnp.float32)
        parts = []
        for h in range(heads):
            lanes = slice(h * block_rows, (h + 1) * block_rows)
            parts.append(summed[h * head_dim : (h + 1) * head_dim, lanes] / row_total[:, lanes])
        gated_t = gate_t * jnp.concatenate(parts, axis=0)
        rows = gated_t.T.reshape(spread, 2, local_rows, channels)
        send_out[block, :, :, column] = rows.astype(jnp.bfloat16)

    def out_copy(block, a, target_core):
        return pltpu.make_async_remote_copy(
            src_ref=send_out.at[block, a, target_core],
            dst_ref=out_ref.at[group],
            send_sem=out_send_sem,
            recv_sem=out_recv_sem,
            device_id={"row": 2 * (a * blocks + block) + target_core},
            device_id_type=MESH,
        )

    def block_step(step, chunk):
        block = lax.rem(chip + step, blocks)
        start, count = chunks[chunk]

        def column_step(column, _):
            attend(column, block)
            return 0

        lax.fori_loop(start, start + count, column_step, 0)
        if chunk < len(chunks) - 1:
            return

        def send(index, _):
            order = index // 2
            jump = spread // 2 + (order // 2 + lax.rem(order, 2)) * (1 - 2 * lax.rem(order, 2))
            target_chip = lax.rem(chip + step + blocks * jump, chips)
            target_core = lax.rem(core + index, 2)

            @pl.when(2 * target_chip + target_core != row)
            def _():
                out_copy(block, target_chip // blocks, target_core).start()

            return 0

        lax.fori_loop(0, 2 * spread, send, 0)

    pltpu.make_async_copy(whole, whole, pair_recv_sem).wait()
    for chunk, (start, count) in enumerate(chunks):
        arrived = send_buf.at[pl.ds(0, chips - 1), pl.ds(0, count)]
        pltpu.make_async_copy(arrived, arrived, a2a_recv_sem.at[chunk]).wait()
        lax.fori_loop(start, start + count, project, 0)

        def chunk_step(step, _, chunk=chunk):
            block_step(step, chunk)
            return 0

        lax.fori_loop(0, blocks, chunk_step, 0)
    out_ref[group] = send_out[lax.rem(chip, blocks), chip // blocks, core]

    ring_blocks = bias.at[mine, pl.ds(0, chips - 1)]
    pltpu.make_async_copy(ring_blocks, ring_blocks, ring_send_sem).wait()
    pltpu.make_async_copy(whole, whole, pair_send_sem).wait()
    pltpu.make_async_copy(others, others, a2a_send_sem).wait()
    received = out_ref.at[pl.ds(0, 2 * chips - 1)]
    pltpu.make_async_copy(received, received, out_send_sem).wait()
    pltpu.make_async_copy(received, received, out_recv_sem).wait()


def on_device(row_count, pair_repr, proj_weight, gate_bias, bias_weight, out_weight, out_bias):
    local_rows, residues, channels = pair_repr.shape
    heads = bias_weight.shape[1]
    inner = proj_weight.shape[1] // 4
    chips = row_count // 2
    width = residues // row_count
    pair_rows = 2 * local_rows
    blocks = residues // LANES
    spread = chips // blocks
    dma = pltpu.SemaphoreType.DMA
    gathered = pl.pallas_call(
        functools.partial(exchange_kernel, chips, heads),
        out_shape=jax.ShapeDtypeStruct((row_count, width, local_rows, channels), jnp.bfloat16),
        in_specs=[pl.BlockSpec(memory_space=pltpu.HBM)] * 4,
        out_specs=pl.BlockSpec(memory_space=pltpu.VMEM),
        scratch_shapes=[
            pltpu.VMEM((channels, 4 * inner), jnp.bfloat16),
            pltpu.VMEM((1, inner), jnp.float32),
            pltpu.VMEM((heads, channels), jnp.bfloat16),
            pltpu.VMEM((2, local_rows, spread, residues // (2 * spread), channels), jnp.bfloat16),
            pltpu.VMEM((residues // 2 * pair_rows, channels), jnp.float32),
            pltpu.VMEM((blocks // 2, 8 * pair_rows, LANES), jnp.float32),
            pltpu.VMEM((chips, width, pair_rows, channels), jnp.bfloat16),
            pltpu.VMEM((width, spread, blocks, pair_rows, channels), jnp.bfloat16),
            pltpu.VMEM((blocks, chips, pair_rows, heads * LANES), jnp.float32),
            pltpu.VMEM((4 * inner, channels), jnp.bfloat16),
            pltpu.VMEM((channels, channels), jnp.float32),
            pltpu.VMEM((width, residues, inner), jnp.bfloat16),
            pltpu.VMEM((width, inner, residues), jnp.bfloat16),
            pltpu.VMEM((blocks, spread, 2, width, local_rows, inner), jnp.bfloat16),
            dma((3,)),
            dma,
            dma,
            dma,
            dma,
            dma((2, chips // 2)),
            dma,
            dma,
            dma,
            dma((2,)),
            dma,
            dma,
        ],
        compiler_params=pltpu.CompilerParams(collective_id=0, has_side_effects=True, vmem_limit_bytes=28 * 2**20),
    )(
        *(
            pltpu.with_memory_space_constraint(array, pltpu.HBM)
            for array in (
                pair_repr.reshape(local_rows, spread, 2, residues // (2 * spread), channels),
                proj_weight,
                gate_bias.reshape(1, inner),
                bias_weight.T,
            )
        )
    )
    gated = gathered.reshape(residues, local_rows, inner)
    update = jnp.einsum("ncf,fz->cnz", gated, out_weight, preferred_element_type=jnp.float32)
    return (update + out_bias).astype(jnp.bfloat16)


def solution(mesh):
    return jax.shard_map(
        functools.partial(on_device, mesh.shape["row"]),
        mesh=mesh,
        in_specs=(P(("group", "row"), None, None), P(), P(), P(), P(), P()),
        out_specs=P(("group", "row"), None, None),
        check_vma=False,
    )
```

```python
import functools

import jax
import jax.numpy as jnp
from jax import lax
from jax.experimental import pallas as pl
from jax.experimental.pallas import tpu as pltpu
from jax.sharding import PartitionSpec as P

EPSILON = 1e-05
MESH = pl.DeviceIdType.MESH
LANES = 128
NT = (((1,), (1,)), ((), ()))


def nt_dot(a, b):
    return lax.dot_general(a, b, NT, preferred_element_type=jnp.float32)


def exchange_kernel(
    chips,
    heads,
    x_ref,
    proj_hbm,
    gate_bias_hbm,
    bias_weight_hbm,
    out_ref,
    proj_ref,
    gate_bias_ref,
    bias_weight_ref,
    xin,
    flat,
    bias_rows,
    send_buf,
    cols,
    bias,
    proj_t,
    gate_col,
    keys,
    values_t,
    result,
    send_out,
    weight_sems,
    in_local_sem,
    in_send_sem,
    in_recv_sem,
    ring_send_sem,
    ring_recv_sem,
    pair_send_sem,
    pair_recv_sem,
    a2a_send_sem,
    a2a_recv_sem,
    out_send_sem,
    out_recv_sem,
):
    local_rows = x_ref.shape[0]
    pair_rows = 2 * local_rows
    blocks = cols.shape[2]
    spread = cols.shape[1]
    width = cols.shape[0]
    channels = x_ref.shape[4]
    half = send_buf.shape[0] * width
    row = lax.axis_index("row")
    chip = row // 2
    core = lax.rem(row, 2)
    partner = row + 1 - 2 * core
    last = chips // 2
    first, tail = width // 2, width // 8
    chunks = ((0, first), (first, width - first - tail), (width - tail, tail))

    def at(distance):
        return lax.rem(row + 2 * distance + 2 * chips, 2 * chips)

    barrier = pltpu.get_barrier_semaphore()
    for other in (partner, at(1), at(-1)):
        pl.semaphore_signal(barrier, inc=1, device_id={"row": other}, device_id_type=MESH)
    keep = pltpu.make_async_copy(x_ref.at[:, :, core], xin.at[core], in_local_sem)
    keep.start()
    weight_copies = [
        pltpu.make_async_copy(source, target, weight_sems.at[i])
        for i, (source, target) in enumerate(
            ((proj_hbm, proj_ref), (gate_bias_hbm, gate_bias_ref), (bias_weight_hbm, bias_weight_ref))
        )
    ]
    for copy in weight_copies:
        copy.start()
    pl.semaphore_wait(barrier, 3)
    swap = pltpu.make_async_remote_copy(
        src_ref=x_ref.at[:, :, 1 - core],
        dst_ref=xin.at[core],
        send_sem=in_send_sem,
        recv_sem=in_recv_sem,
        device_id={"row": partner},
        device_id_type=MESH,
    )
    swap.start()
    for copy in weight_copies:
        copy.wait()

    proj_t[...] = proj_ref[...].astype(jnp.float32).T.astype(jnp.bfloat16)
    gate_col[...] = jnp.broadcast_to(gate_bias_ref[...], (channels, channels)).T
    bias_w = bias_weight_ref[...].astype(jnp.float32)
    bias_w = jnp.concatenate([bias_w, jnp.zeros((8 - heads, channels), jnp.float32)], axis=0).astype(jnp.bfloat16)

    keep.wait()

    def normalize_row(part, line):
        index = part * local_rows + line
        x = xin[part, line].reshape(half, channels).astype(jnp.float32)
        centred = x - jnp.mean(x, axis=-1, keepdims=True)
        variance = jnp.mean(centred * centred, axis=-1, keepdims=True)
        normed = centred * lax.rsqrt(variance + EPSILON)
        rounded = normed.astype(jnp.bfloat16)
        groups = [rounded[g * pair_rows : (g + 1) * pair_rows] for g in range(half // pair_rows)]
        ordered = [groups[a * (blocks // 2) + block] for block in range(blocks // 2) for a in range(spread)]
        row_bias = nt_dot(bias_w, jnp.concatenate(ordered, axis=0))
        for block in range(blocks // 2):
            lanes = slice(block * LANES, (block + 1) * LANES)
            bias_rows[block, pl.ds(pl.multiple_of(index * 8, 8), 8), :] = row_bias[:, lanes]
        flat[pl.ds(index, half, stride=pair_rows), :] = normed

    def own_row(line, _):
        normalize_row(core, line)
        return 0

    def other_row(line, _):
        normalize_row(1 - core, line)
        return 0

    lax.fori_loop(0, local_rows, own_row, 0)
    swap.wait()
    lax.fori_loop(0, local_rows, other_row, 0)
    for block in range(blocks // 2):
        for h in range(heads):
            piece = bias_rows[block, pl.ds(h, pair_rows, stride=8), :]
            bias[core * (blocks // 2) + block, chip, :, h * LANES : (h + 1) * LANES] = piece

    mine = pl.ds(core * (blocks // 2), blocks // 2)

    def ring_copy(source, step, direction, target):
        ref = bias.at[mine, source]
        return pltpu.make_async_remote_copy(
            src_ref=ref,
            dst_ref=ref,
            send_sem=ring_send_sem,
            recv_sem=ring_recv_sem.at[direction, step],
            device_id={"row": target},
            device_id_type=MESH,
        )

    def pair_copy(source):
        ref = bias.at[mine, source]
        return pltpu.make_async_remote_copy(
            src_ref=ref,
            dst_ref=ref,
            send_sem=pair_send_sem,
            recv_sem=pair_recv_sem,
            device_id={"row": partner},
            device_id_type=MESH,
        )

    def column_copy(distance, chunk):
        target = at(distance)
        part = pl.ds(*chunks[chunk])
        return pltpu.make_async_remote_copy(
            src_ref=send_buf.at[target // 2, part],
            dst_ref=cols.at[part, chip // blocks, lax.rem(chip, blocks)],
            send_sem=a2a_send_sem,
            recv_sem=a2a_recv_sem.at[chunk],
            device_id={"row": target},
            device_id_type=MESH,
        )

    ring_copy(chip, 0, 0, at(1)).start()
    ring_copy(chip, 0, 1, at(-1)).start()
    pair_copy(chip).start()

    def round_chunk(index, _):
        rows = width * pair_rows
        piece = flat[pl.ds(pl.multiple_of(index * rows, rows), rows), :]
        send_buf[index] = piece.reshape(width, pair_rows, channels).astype(jnp.bfloat16)
        return 0

    lax.fori_loop(0, chips, round_chunk, 0)
    cols[:, chip // blocks, lax.rem(chip, blocks)] = send_buf[chip]

    def chip_at(distance):
        return at(distance) // 2

    def ring_step(step, _):
        behind, ahead = chip_at(-step), chip_at(step)
        ring_copy(behind, step - 1, 0, at(1)).wait_recv()
        ring_copy(behind, step, 0, at(1)).start()
        ring_copy(ahead, step - 1, 1, at(-1)).wait_recv()

        @pl.when(step < last - 1)
        def _():
            ring_copy(ahead, step, 1, at(-1)).start()

        pair_copy(behind).start()
        pair_copy(ahead).start()
        column_copy(step, 0).start()
        column_copy(-step, 0).start()
        return 0

    lax.fori_loop(1, last, ring_step, 0)
    opposite = chip_at(-last)
    ring_copy(opposite, last - 1, 0, at(1)).wait_recv()
    pair_copy(opposite).start()
    column_copy(last, 0).start()
    for chunk in range(1, len(chunks)):
        column_copy(last, chunk).start()

        def send_columns(nearer, _, chunk=chunk):
            column_copy(last - nearer, chunk).start()
            column_copy(nearer - last, chunk).start()
            return 0

        lax.fori_loop(1, last, send_columns, 0)

    whole = bias.at[mine]
    others = send_buf.at[pl.ds(0, chips - 1)]

    inner = proj_t.shape[0] // 4
    head_dim = inner // heads
    residues = chips * pair_rows
    block_rows = spread * pair_rows

    def project(column, _):
        x = cols[column].reshape(residues, channels)
        keys[column] = nt_dot(x, proj_t[inner : 2 * inner]).astype(jnp.bfloat16)
        values_t[column] = nt_dot(proj_t[2 * inner : 3 * inner], x).astype(jnp.bfloat16)
        return 0

    head_of_row = lax.broadcasted_iota(jnp.int32, (inner, block_rows), 0) // head_dim
    group = (chip // blocks) * (2 * blocks) + core * blocks + lax.rem(chip, blocks)

    def attend(column, block):
        x = cols[column, :, block].reshape(block_rows, channels)
        query_t = nt_dot(proj_t[0:inner], x) * head_dim ** (-0.5)
        gate_t = jax.nn.sigmoid(nt_dot(proj_t[3 * inner : 4 * inner], x) + gate_col[...])
        spread_q = jnp.concatenate(
            [jnp.where(head_of_row == h, query_t, 0.0).astype(jnp.bfloat16) for h in range(heads)], axis=1
        )
        scores = jnp.dot(keys[column], spread_q, preferred_element_type=jnp.float32)
        scores = scores + bias[block].reshape(residues, heads * block_rows)
        row_max = jnp.max(scores, axis=0, keepdims=True)
        expd = jnp.exp(scores - row_max)
        row_total = jnp.sum(expd, axis=0, keepdims=True)
        summed = jnp.dot(values_t[column], expd.astype(jnp.bfloat16), preferred_element_type=jnp.float32)
        parts = []
        for h in range(heads):
            lanes = slice(h * block_rows, (h + 1) * block_rows)
            parts.append(summed[h * head_dim : (h + 1) * head_dim, lanes] / row_total[:, lanes])
        gated_t = gate_t * jnp.concatenate(parts, axis=0)
        result[block, pl.ds(column, block_rows, stride=width), :] = gated_t.T

    def out_copy(block, a, target_core):
        target_chip = a * blocks + block
        return pltpu.make_async_remote_copy(
            src_ref=send_out.at[block, a, target_core],
            dst_ref=out_ref.at[:, group],
            send_sem=out_send_sem,
            recv_sem=out_recv_sem,
            device_id={"row": 2 * target_chip + target_core},
            device_id_type=MESH,
        )

    def attend_block(step, chunk):
        block = lax.rem(chip + step, blocks)
        start, count = chunks[chunk]

        def column_step(column, _):
            attend(column, block)
            return 0

        lax.fori_loop(start, start + count, column_step, 0)
        return block

    def send_block(step, _):
        block = attend_block(step, len(chunks) - 1)
        send_out[block] = result[block].reshape(spread, 2, local_rows, width, channels).astype(jnp.bfloat16)

        def send(index, _):
            order = index // 2
            jump = spread // 2 + (order // 2 + lax.rem(order, 2)) * (1 - 2 * lax.rem(order, 2))
            target_chip = lax.rem(chip + step + blocks * jump, chips)
            target_core = lax.rem(core + index, 2)

            @pl.when(2 * target_chip + target_core != row)
            def _():
                out_copy(block, target_chip // blocks, target_core).start()

            return 0

        lax.fori_loop(0, 2 * spread, send, 0)
        return 0

    pltpu.make_async_copy(whole, whole, pair_recv_sem).wait()
    for chunk, (start, count) in enumerate(chunks):
        arrived = send_buf.at[pl.ds(0, chips - 1), pl.ds(0, count)]
        pltpu.make_async_copy(arrived, arrived, a2a_recv_sem.at[chunk]).wait()
        lax.fori_loop(start, start + count, project, 0)
        if chunk < len(chunks) - 1:

            def attend_early(step, _, chunk=chunk):
                attend_block(step, chunk)
                return 0

            lax.fori_loop(0, blocks, attend_early, 0)
    lax.fori_loop(0, blocks, send_block, 0)
    out_ref[:, group] = send_out[lax.rem(chip, blocks), chip // blocks, core]

    ring_blocks = bias.at[mine, pl.ds(0, chips - 1)]
    pltpu.make_async_copy(ring_blocks, ring_blocks, ring_send_sem).wait()
    pltpu.make_async_copy(whole, whole, pair_send_sem).wait()
    pltpu.make_async_copy(others, others, a2a_send_sem).wait()
    received = out_ref.at[:, pl.ds(0, 2 * chips - 1)]
    pltpu.make_async_copy(received, received, out_send_sem).wait()
    pltpu.make_async_copy(received, received, out_recv_sem).wait()


def on_device(row_count, pair_repr, proj_weight, gate_bias, bias_weight, out_weight, out_bias):
    local_rows, residues, channels = pair_repr.shape
    heads = bias_weight.shape[1]
    inner = proj_weight.shape[1] // 4
    chips = row_count // 2
    width = residues // row_count
    pair_rows = 2 * local_rows
    blocks = residues // LANES
    spread = chips // blocks
    dma = pltpu.SemaphoreType.DMA
    gathered = pl.pallas_call(
        functools.partial(exchange_kernel, chips, heads),
        out_shape=jax.ShapeDtypeStruct((local_rows, row_count, width, channels), jnp.bfloat16),
        in_specs=[pl.BlockSpec(memory_space=pltpu.HBM)] * 4,
        out_specs=pl.BlockSpec(memory_space=pltpu.VMEM),
        scratch_shapes=[
            pltpu.VMEM((channels, 4 * inner), jnp.bfloat16),
            pltpu.VMEM((1, inner), jnp.float32),
            pltpu.VMEM((heads, channels), jnp.bfloat16),
            pltpu.VMEM((2, local_rows, spread, residues // (2 * spread), channels), jnp.bfloat16),
            pltpu.VMEM((residues // 2 * pair_rows, channels), jnp.float32),
            pltpu.VMEM((blocks // 2, 8 * pair_rows, LANES), jnp.float32),
            pltpu.VMEM((chips, width, pair_rows, channels), jnp.bfloat16),
            pltpu.VMEM((width, spread, blocks, pair_rows, channels), jnp.bfloat16),
            pltpu.VMEM((blocks, chips, pair_rows, heads * LANES), jnp.float32),
            pltpu.VMEM((4 * inner, channels), jnp.bfloat16),
            pltpu.VMEM((channels, channels), jnp.float32),
            pltpu.VMEM((width, residues, inner), jnp.bfloat16),
            pltpu.VMEM((width, inner, residues), jnp.bfloat16),
            pltpu.VMEM((blocks, LANES * width, inner), jnp.float32),
            pltpu.VMEM((blocks, spread, 2, local_rows, width, inner), jnp.bfloat16),
            dma((3,)),
            dma,
            dma,
            dma,
            dma,
            dma((2, chips // 2)),
            dma,
            dma,
            dma,
            dma((3,)),
            dma,
            dma,
        ],
        compiler_params=pltpu.CompilerParams(collective_id=0, has_side_effects=True, vmem_limit_bytes=28 * 2**20),
    )(
        *(
            pltpu.with_memory_space_constraint(array, pltpu.HBM)
            for array in (
                pair_repr.reshape(local_rows, spread, 2, residues // (2 * spread), channels),
                proj_weight,
                gate_bias.reshape(1, inner),
                bias_weight.T,
            )
        )
    )
    gated = gathered.reshape(local_rows, residues, inner)
    update = jnp.einsum("cnf,fz->cnz", gated, out_weight, preferred_element_type=jnp.float32)
    return (update + out_bias).astype(jnp.bfloat16)


def solution(mesh):
    return jax.shard_map(
        functools.partial(on_device, mesh.shape["row"]),
        mesh=mesh,
        in_specs=(P(("group", "row"), None, None), P(), P(), P(), P(), P()),
        out_specs=P(("group", "row"), None, None),
        check_vma=False,
    )
```
